256 devices in a mesh: grp: 4 (over y, x), path: 32 (over z), amp: 2 (over core).
Axes of the slice: x: 2, y: 2, z: 32, core: 2. Of those that a mesh axis runs over, the one named last changes fastest.
The devices are a block of a 4x8x32 slice.
Arguments:
- left_slabs: bfloat16 [2048, 2, 16384], P(('grp', 'path'), None, 'amp'), parts along dimension 0, may hold values from -0.59765625 to 0.59765625
- right_slabs: bfloat16 [2048, 2, 8192], P(('grp', 'path'), None, 'amp'), parts along dimension 0, may hold values from -0.59765625 to 0.59765625
- term_index: int32 [2048], P(('grp', 'path')), parts along dimension 0, may hold values from 0 to 3
- left_terms: float32 [4, 2, 2, 2], replicated, may hold values from -4.2 to 4.2
- right_terms: float32 [4, 2, 2, 2], replicated, may hold values from -4.2 to 4.2
- left_gates: bfloat16 [2, 2, 128, 128], replicated, may hold values from -0.375 to 0.375
- right_gates: bfloat16 [2, 2, 128, 128], replicated, may hold values from -0.375 to 0.375
Outputs:
- amplitudes: bfloat16 [2, 65536, 8192], P(None, ('grp', 'path'), 'amp'), parts along dimension 1
The draws below stay inside these ranges and needn't reach their ends.
There are 4 independent parts, one for each index of `grp`. The reference program is written for one: setup_inputs(seed, part) draws one part's arguments, and reference() takes and returns one part's arrays. A program takes and returns all parts, laid end to end along the dimension named above; an argument that names none is the same for every part. Nothing has to cross between parts.
All inputs are finite; a program needn't handle non-finite values.
Results may differ from the reference program's by a relative error of at most 0.0081.
Values may be sent and summed in bfloat16 or wider, within the bound.
A program may use at most 128 MiB of HBM per device.

```python
import jax
import jax.numpy as jnp
from jax import lax

GATE = 128
TERMS = 4
LA = 16384
RA = 8192
PATHS = 512


def place_ends(drawn, own_key, smallest, high):
    place = [jax.random.randint(jax.random.fold_in(own_key, axis), (), 0, length) for axis, length in enumerate(drawn.shape)]
    main_axis = drawn.shape.index(max(drawn.shape))
    beside = place[:main_axis] + [(place[main_axis] + 1) % drawn.shape[main_axis]] + place[main_axis + 1:]
    return drawn.at[tuple(place)].set(smallest).at[tuple(beside)].set(high)


def level_of(stream_key, extent, split, least, high):
    gain, own = 1.0, jax.random.fold_in(stream_key, 6)
    for axis_at, blocks in split:
        steps = jnp.exp(jax.random.uniform(jax.random.fold_in(own, axis_at), (blocks,), jnp.float32, least / len(split), high / len(split)))
        gain = gain * jnp.repeat(steps, extent[axis_at] // blocks).reshape([-1 if axis == axis_at else 1 for axis in range(len(extent))])
    return gain


def gaussian(stream_key, dims, width, reach, shards=(), kind=jnp.bfloat16):
    level = level_of(stream_key, dims, shards, -0.22, 0.18) if shards else 1.0
    values = jax.random.normal(stream_key, dims, jnp.float32) * width * level
    return jnp.minimum(jnp.maximum(values, -reach), reach).astype(kind)


def setup_inputs(seed: int = 0, part: int = 0) -> dict:
    key_list = jax.random.split(jax.random.key(seed), 8)
    part_keys = jax.random.split(jax.random.fold_in(key_list[7], part), 8)
    return {
        "left_slabs": gaussian(part_keys[0], (PATHS, 2, LA), 0.1, 0.59765625, ((0, 32), (2, 2))),
        "right_slabs": gaussian(part_keys[1], (PATHS, 2, RA), 0.1, 0.59765625, ((0, 32), (2, 2))),
        "term_index": place_ends(jax.random.randint(part_keys[2], (PATHS,), 0, TERMS), jax.random.fold_in(part_keys[2], 1), 0, TERMS - 1).astype(jnp.int32),
        "left_terms": gaussian(key_list[3], (TERMS, 2, 2, 2), 0.7, 4.2, (), jnp.float32),
        "right_terms": gaussian(key_list[4], (TERMS, 2, 2, 2), 0.7, 4.2, (), jnp.float32),
        "left_gates": gaussian(key_list[5], (2, 2, GATE, GATE), (2 * GATE) ** -0.5, 0.375),
        "right_gates": gaussian(key_list[6], (2, 2, GATE, GATE), (2 * GATE) ** -0.5, 0.375),
    }


def cut_term(slab, term_mix):
    paths_here, _, length = slab.shape
    values = slab.astype(jnp.float32).reshape(paths_here, 2, length // 2, 2)
    real_rows = values[:, 0]
    imag_rows = values[:, 1]
    real_mix = term_mix[:, 0]
    imag_mix = term_mix[:, 1]
    real_part = jnp.einsum('pkj,pmj->pkm', real_rows, real_mix) - jnp.einsum('pkj,pmj->pkm', imag_rows, imag_mix)
    imag_part = jnp.einsum('pkj,pmj->pkm', real_rows, imag_mix) + jnp.einsum('pkj,pmj->pkm', imag_rows, real_mix)
    return jnp.stack([real_part, imag_part], 1).reshape(paths_here, 2, length).astype(jnp.bfloat16)


def apply_low(slab, gate_mat):
    paths_here, _, length = slab.shape
    gate_width = gate_mat.shape[-1]
    real_rows = slab[:, 0].reshape(-1, gate_width)
    imag_rows = slab[:, 1].reshape(-1, gate_width)
    upper = jnp.concatenate([gate_mat[0].T, gate_mat[1].T], 1)
    lower = jnp.concatenate([-gate_mat[1].T, gate_mat[0].T], 1)
    right_matrix = jnp.concatenate([upper, lower], 0)
    product = jnp.dot(jnp.concatenate([real_rows, imag_rows], 1), right_matrix, preferred_element_type=jnp.float32)
    real_part = product[:, :gate_width].reshape(paths_here, length)
    imag_part = product[:, gate_width:].reshape(paths_here, length)
    return jnp.stack([real_part, imag_part], 1).astype(jnp.bfloat16)


def apply_high(grouped, gate_mat):
    gate_width = gate_mat.shape[-1]
    stacked = jnp.concatenate([grouped[:, 0], grouped[:, 1]], 1)
    upper = jnp.concatenate([gate_mat[0], -gate_mat[1]], 1)
    lower = jnp.concatenate([gate_mat[1], gate_mat[0]], 1)
    left_matrix = jnp.concatenate([upper, lower], 0)
    product = jnp.einsum('mk,nkr->nmr', left_matrix.astype(jnp.float32), stacked.astype(jnp.float32))
    return jnp.stack([product[:, :gate_width], product[:, gate_width:]], 1).astype(jnp.bfloat16)


def contract(left_part, right_part):
    left_stack = jnp.concatenate([left_part[:, 0], left_part[:, 1]], 0)
    right_real = jnp.concatenate([right_part[:, 0], -right_part[:, 1]], 0)
    right_imag = jnp.concatenate([right_part[:, 1], right_part[:, 0]], 0)
    contract_dims = (((0,), (0,)), ((), ()))
    real_part = lax.dot_general(left_stack, right_real, contract_dims, preferred_element_type=jnp.float32)
    imag_part = lax.dot_general(left_stack, right_imag, contract_dims, preferred_element_type=jnp.float32)
    return real_part, imag_part


def mixes(term_index, terms):
    chosen = (term_index[:, None] == jnp.arange(terms.shape[0], dtype=jnp.int32)[None, :]).astype(jnp.float32)
    flat = jnp.dot(chosen, terms.reshape(terms.shape[0], 8), precision=lax.Precision.HIGHEST)
    return flat.reshape(-1, 2, 2, 2)


def reference(left_slabs, right_slabs, term_index, left_terms, right_terms, left_gates, right_gates):
    paths_all = left_slabs.shape[0]
    left = cut_term(left_slabs, mixes(term_index, left_terms))
    left = apply_low(left, left_gates[0])
    left = apply_high(left.reshape(paths_all, 2, GATE, LA // GATE), left_gates[1]).reshape(paths_all, 2, LA)
    right = cut_term(right_slabs, mixes(term_index, right_terms))
    right = apply_low(right, right_gates[0])
    right = apply_high(right.reshape(paths_all, 2, GATE, RA // GATE), right_gates[1]).reshape(paths_all, 2, RA)
    real_part, imag_part = contract(left, right)
    return jnp.stack([real_part, imag_part], 0).astype(jnp.bfloat16)
```

```python
import functools

import jax
import jax.numpy as jnp
from jax import lax
from jax.experimental import pallas as pl
from jax.experimental.pallas import tpu as pltpu
from jax.sharding import PartitionSpec as P

MESH = pl.DeviceIdType.MESH
F32 = jnp.float32
BF16 = jnp.bfloat16
PIECES = 4
NT = (((1,), (1,)), ((), ()))
TN = (((0,), (0,)), ((), ()))


def dot(a, b, dims=(((1,), (0,)), ((), ()))):
    return lax.dot_general(a, b, dims, preferred_element_type=F32)


def grid2(rows, cols):
    return (
        lax.broadcasted_iota(jnp.int32, (rows, cols), 0),
        lax.broadcasted_iota(jnp.int32, (rows, cols), 1),
    )


def one_hot(cond):
    return jnp.where(cond, 1.0, 0.0).astype(BF16)


def stack_matrix(re, im):
    upper = jnp.concatenate([re, -im], 1)
    lower = jnp.concatenate([im, re], 1)
    return jnp.concatenate([upper, lower], 0)


def coefficients(idx_ref, term_ref, path, even):
    base = idx_ref[path] * 8
    pick = lambda c, m, j: term_ref[base + (c * 4 + m * 2 + j)]
    spread = lambda s0, s1: jnp.where(even, s0, s1)
    return (
        spread(pick(0, 0, 0), pick(0, 1, 1)),
        spread(pick(1, 0, 0), pick(1, 1, 1)),
        spread(pick(0, 0, 1), pick(0, 1, 0)),
        spread(pick(1, 0, 1), pick(1, 1, 0)),
    )


def cut_paths(slab, first_path, idx_ref, term_ref, pair_swap, even):
    paths, _, rows, width = slab.shape
    flat = slab.reshape(paths * 2 * rows, width)
    swapped = dot(flat, pair_swap)
    wide = flat.astype(F32)
    done = []
    for p in range(paths):
        at = 2 * p * rows
        xr, xi = wide[at : at + rows], wide[at + rows : at + 2 * rows]
        sr, si = swapped[at : at + rows], swapped[at + rows : at + 2 * rows]
        ar, ai, br, bi = coefficients(idx_ref, term_ref, first_path + p, even)
        cr = (xr * ar + sr * br) - (xi * ai + si * bi)
        ci = (xr * ai + sr * bi) + (xi * ar + si * br)
        done.append(jnp.concatenate([cr, ci], 1).astype(BF16))
    return jnp.concatenate(done, 0)


def exchange_kernel(
    chips,
    idx_ref, lterm_ref, rterm_ref,
    left_ref, right_ref, lgate_ref, rgate_ref,
    lall_ref, rall_ref,
    lx, rx, lt, rt, lsend, rown, up, down,
    swap_send, swap_recv,
    ag_send, ag_recv, aa_send, aa_recv, pr_send, pr_recv, loc_sem, rloc_sem,
):
    me = lax.axis_index("path")
    core = lax.axis_index("amp")
    nxt, prv = lax.rem(me + 1, chips), lax.rem(me + chips - 1, chips)
    peer = {"amp": 1 - core}
    toward = ({"path": nxt}, {"path": prv})
    half = chips // 2
    pieces = rown.shape[0]

    barrier = pltpu.get_barrier_semaphore()
    for who in (peer, *toward):
        pl.semaphore_signal(barrier, inc=1, device_id=who, device_id_type=MESH)
    pl.semaphore_wait(barrier, 3)

    mine = lx.shape[0]
    lrows, rrows = left_ref.shape[2], right_ref.shape[2]
    rplace = pl.ds(pl.multiple_of(core * rrows, rrows), rrows)
    lplace = pl.ds(pl.multiple_of(core * lrows, lrows), lrows)
    give_right = pltpu.make_async_remote_copy(
        src_ref=right_ref, dst_ref=rx.at[:, :, rplace],
        send_sem=swap_send.at[0], recv_sem=swap_recv.at[0], device_id=peer, device_id_type=MESH)
    give_left = pltpu.make_async_remote_copy(
        src_ref=left_ref.at[pl.ds((1 - core) * mine, mine)], dst_ref=lx.at[:, :, lplace],
        send_sem=swap_send.at[1], recv_sem=swap_recv.at[1], device_id=peer, device_id_type=MESH)
    give_right.start()
    give_left.start()
    rx[:, :, rplace] = right_ref[...]
    lx[:, :, lplace] = left_ref[pl.ds(core * mine, mine)]

    row, col = grid2(128, 128)
    pair_swap = one_hot(row == (col ^ 1))
    even = (lax.broadcasted_iota(jnp.int32, (1, 128), 1) & 1) == 0
    prow, pcol = grid2(256, 256)
    regroup = one_hot(pcol == (prow % 8) * 32 + prow // 8)

    s_low = stack_matrix(rgate_ref[0, 0], rgate_ref[0, 1])
    s_low = jnp.concatenate(
        [s_low, s_low[64:128], s_low[0:64], s_low[192:256], s_low[128:192]], 0)
    here = rrows
    full = 2 * here
    srow, scol = grid2(here, 128)
    krow, kcol = grid2(2 * full, 128)
    parts = []
    for c in range(2):
        gate = rgate_ref[1, c]
        rows_of = []
        for t in range(2):
            pick_rows = one_hot(scol == 2 * (core * here + srow) + t)
            pick_cols = one_hot(kcol == 2 * (krow % full) + (krow // full + t) % 2)
            some = dot(pick_rows, gate).astype(BF16)
            rows_of.append(dot(some, pick_cols, NT).astype(BF16))
        parts.append(jnp.concatenate(rows_of, 0))
    s_high = stack_matrix(parts[0], parts[1])

    give_right.wait_recv()
    low_lanes = lax.broadcasted_iota(jnp.int32, (1, 128), 1) < 64
    step = 4
    for first in range(0, rx.shape[0], step):
        cut = cut_paths(rx[first : first + step], first, idx_ref, rterm_ref, pair_swap, even)
        low = dot(cut, s_low, NT).astype(BF16)
        tall = []
        for p in range(step):
            at = low[p * full : (p + 1) * full]
            tall.append(jnp.concatenate(
                [at[:, 0:128], at[:, 256:384], at[:, 128:256], at[:, 384:512]], 0))
        turned = dot(s_high, jnp.concatenate(tall, 1))
        for p in range(step):
            z = turned[:, p * 128 : (p + 1) * 128]
            q = first + p
            for c in range(2):
                at = 2 * c * here
                pair = jnp.where(low_lanes, z[at : at + here], z[at + here : at + 2 * here])
                rt[c, q // 8, (q % 8) * 32 : (q % 8) * 32 + here] = pair.astype(BF16)
    per_piece = here // pieces
    for g in range(2):
        both = [dot(regroup, rt[c, g]) for c in range(2)]
        for r in range(here):
            tile = jnp.concatenate([b[r * 8 : r * 8 + 8] for b in both], 0).astype(BF16)
            at = (r % per_piece) * 128
            rown[r // per_piece, g * 16 : g * 16 + 16, at : at + 128] = tile

    def chunk(d, s):
        return lax.rem(me + (chips - s if d == 0 else s), chips)

    def gather_copy(d, s, j):
        at = chunk(d, s)
        src = rown.at[j] if s == 0 else rall_ref.at[at, j]
        return pltpu.make_async_remote_copy(
            src_ref=src, dst_ref=rall_ref.at[at, j],
            send_sem=ag_send.at[d, s, j], recv_sem=ag_recv.at[d, s, j],
            device_id=toward[d], device_id_type=MESH)

    def gather_arrival(d, s, j):
        at = chunk(d, s + 1)
        return pltpu.make_async_remote_copy(
            src_ref=rall_ref.at[at, j], dst_ref=rall_ref.at[at, j],
            send_sem=ag_send.at[d, s, j], recv_sem=ag_recv.at[d, s, j],
            device_id=toward[d], device_id_type=MESH)

    gather_steps = (half - 1, half)

    def gather_step(s):
        @pl.loop(0, pieces)
        def _(j):
            for d in range(2):
                if 1 <= s <= gather_steps[d]:
                    gather_arrival(d, s - 1, j).wait_recv()
                if s < gather_steps[d]:
                    gather_copy(d, s, j).start()

    gather_step(0)
    keep_own = pltpu.make_async_copy(rown, rall_ref.at[me], rloc_sem)
    keep_own.start()

    s_low = stack_matrix(lgate_ref[0, 0], lgate_ref[0, 1])
    s_high = stack_matrix(lgate_ref[1, 0], lgate_ref[1, 1])
    give_left.wait_recv()
    step = 2
    groups = 4
    for first in range(0, mine, step):
        cut = cut_paths(
            lx[first : first + step], core * mine + first, idx_ref, lterm_ref, pair_swap, even)
        low = dot(cut, s_low, NT).astype(BF16)
        tall = [
            jnp.concatenate([low[p * 128 : (p + 1) * 128, c * 128 : (c + 1) * 128] for c in range(2)], 0)
            for p in range(step)
        ]
        turned = dot(s_high, jnp.concatenate(tall, 1)).astype(BF16)
        for p in range(step):
            for c in range(2):
                for g in range(groups):
                    at = c * 128 + g * 32
                    lt[c, g, (first + p) * 32 : (first + p) * 32 + 32] = (
                        turned[at : at + 32, p * 128 : (p + 1) * 128])
    per_chip = 128 // chips
    for g in range(groups):
        both = [dot(regroup, lt[c, g]) for c in range(2)]
        for r in range(32):
            m = g * 32 + r
            tile = jnp.concatenate([b[r * 8 : r * 8 + 8] for b in both], 0).astype(BF16)
            slot = lax.rem(m // per_chip - me + chips, chips)
            at = (m % per_chip) * 128
            lsend[slot, :, at : at + 128] = tile

    counts = ([half - s for s in range(half)], [half - 1 - s for s in range(half - 1)])
    bases = [[sum(c[:s]) for s in range(len(c))] for c in counts]
    landing = (up, down)

    def block_copy(d, s):
        n = counts[d][s]
        if s == 0:
            src = lsend.at[pl.ds(1, n)] if d == 0 else lsend.at[pl.ds(half + 1, n)]
        else:
            src = landing[d].at[pl.ds(bases[d][s - 1] + (1 if d == 0 else 0), n)]
        return pltpu.make_async_remote_copy(
            src_ref=src, dst_ref=landing[d].at[pl.ds(bases[d][s], n)],
            send_sem=aa_send.at[d, s], recv_sem=aa_recv.at[d, s],
            device_id=toward[d], device_id_type=MESH)

    def keep(src, at, n):
        here_copy = pltpu.make_async_copy(src, lall_ref.at[at, core], loc_sem.at[n])
        there_copy = pltpu.make_async_remote_copy(
            src_ref=src, dst_ref=lall_ref.at[at, core],
            send_sem=pr_send.at[n], recv_sem=pr_recv.at[n], device_id=peer, device_id_type=MESH)
        here_copy.start()
        there_copy.start()
        return here_copy, there_copy

    kept = []
    for s in range(half + 1):
        if s >= 1:
            gather_step(s)
        for d in range(2):
            if 1 <= s <= len(counts[d]):
                block_copy(d, s - 1).wait_recv()
            if s < len(counts[d]):
                block_copy(d, s).start()
            if s == 0 and d == 0:
                kept.append(keep(lsend.at[0], me, 0))
            if 1 <= s <= len(counts[d]):
                at = bases[d][s - 1] + (0 if d == 0 else counts[d][s - 1] - 1)
                kept.append(keep(landing[d].at[at], chunk(d, s), len(kept)))

    give_right.wait_send()
    give_left.wait_send()
    keep_own.wait()
    for s in range(half):
        @pl.loop(0, pieces)
        def _(j):
            for d in range(2):
                if s < gather_steps[d]:
                    gather_copy(d, s, j).wait_send()
        for d in range(2):
            if s < len(counts[d]):
                block_copy(d, s).wait_send()
    for here_copy, there_copy in kept:
        here_copy.wait()
        there_copy.wait()


def product_kernel(left_ref, right_ref, out_ref, lhs):
    rows = left_ref.shape[1]
    depth = left_ref.shape[0]

    @pl.when((pl.program_id(0) == 0) & (pl.program_id(1) == 0))
    def _():
        row, col = grid2(256, 256)
        imag = (row // 8) % 2 == 1
        signed = jnp.where(row == col, jnp.where(imag, -1.0, 1.0), 0.0).astype(BF16)
        crossed = one_hot(row == (col ^ 8))
        for k in range(0, depth, 256):
            part = left_ref[k : k + 256]
            lhs[0:rows, k : k + 256] = dot(part, signed, TN).astype(BF16)
            lhs[rows : 2 * rows, k : k + 256] = dot(part, crossed, TN).astype(BF16)

    right = right_ref[...].reshape(depth, right_ref.shape[-1])
    out_ref[0] = dot(lhs[0:rows], right).astype(BF16)
    out_ref[1] = dot(lhs[rows : 2 * rows], right).astype(BF16)


def shards(left_slabs, right_slabs, term_index, left_terms, right_terms, left_gates, right_gates):
    chips = lax.axis_size("path")
    paths = left_slabs.shape[0]
    mine = paths // 2
    left = left_slabs.reshape(paths, 2, -1, 128)
    right = right_slabs.reshape(paths, 2, -1, 128)
    lrows, rrows = left.shape[2], right.shape[2]
    half = chips // 2
    pieces = PIECES
    cols = rrows * 128
    block = 2 * lrows * 128 // chips
    vmem = pl.BlockSpec(memory_space=pltpu.VMEM)
    smem = pl.BlockSpec(memory_space=pltpu.SMEM)
    hbm = pl.BlockSpec(memory_space=pl.ANY)
    dma = pltpu.SemaphoreType.DMA
    left_all, right_all = pl.pallas_call(
        functools.partial(exchange_kernel, chips),
        out_shape=(
            jax.ShapeDtypeStruct((chips, 2, 2 * mine, block), BF16),
            jax.ShapeDtypeStruct((chips, pieces, 2 * paths, cols // pieces), BF16),
        ),
        in_specs=[smem, smem, smem, vmem, vmem, vmem, vmem],
        out_specs=(hbm, hbm),
        scratch_shapes=[
            pltpu.VMEM((mine, 2, 2 * lrows, 128), BF16),
            pltpu.VMEM((paths, 2, 2 * rrows, 128), BF16),
            pltpu.VMEM((2, 4, 256, 128), BF16),
            pltpu.VMEM((2, 2, 256, 128), BF16),
            pltpu.VMEM((chips, 2 * mine, block), BF16),
            pltpu.VMEM((pieces, 2 * paths, cols // pieces), BF16),
            pltpu.VMEM((half * (half + 1) // 2, 2 * mine, block), BF16),
            pltpu.VMEM((half * (half - 1) // 2, 2 * mine, block), BF16),
            dma((2,)), dma((2,)),
            dma((2, half, pieces)), dma((2, half, pieces)),
            dma((2, half)), dma((2, half)),
            dma((chips,)), dma((chips,)), dma((chips,)), dma,
        ],
        compiler_params=pltpu.CompilerParams(
            collective_id=0, has_side_effects=True, vmem_limit_bytes=40 * 1024 * 1024),
        name="exchange",
    )(
        term_index, left_terms.reshape(-1), right_terms.reshape(-1),
        left, right, left_gates, right_gates,
    )
    depth = chips * 2 * paths
    tile = min(512, cols // pieces)
    per = cols // pieces // tile
    return pl.pallas_call(
        product_kernel,
        grid=(pieces, per),
        out_shape=jax.ShapeDtypeStruct((2, block, cols), BF16),
        in_specs=[
            pl.BlockSpec((depth, block), lambda j, k: (0, 0)),
            pl.BlockSpec((chips, 1, 2 * paths, tile), lambda j, k: (0, j, 0, k)),
        ],
        out_specs=pl.BlockSpec((2, block, tile), lambda j, k: (0, 0, j * per + k)),
        scratch_shapes=[pltpu.VMEM((2 * block, depth), BF16)],
        compiler_params=pltpu.CompilerParams(vmem_limit_bytes=40 * 1024 * 1024),
        name="product",
    )(left_all.reshape(depth, block), right_all)


def solution(mesh):
    return jax.shard_map(
        shards,
        mesh=mesh,
        in_specs=(
            P(("grp", "path"), None, "amp"),
            P(("grp", "path"), None, "amp"),
            P(("grp", "path")),
            P(),
            P(),
            P(),
            P(),
        ),
        out_specs=P(None, ("grp", "path"), "amp"),
        check_vma=False,
    )
```

```python
import functools

import jax
import jax.numpy as jnp
from jax import lax
from jax.experimental import pallas as pl
from jax.experimental.pallas import tpu as pltpu
from jax.sharding import PartitionSpec as P

MESH = pl.DeviceIdType.MESH
F32 = jnp.float32
BF16 = jnp.bfloat16
VMEM_LIMIT = 24 * 1024 * 1024
NT = (((1,), (1,)), ((), ()))
TN = (((0,), (0,)), ((), ()))


def dot(a, b, dims=(((1,), (0,)), ((), ()))):
    return lax.dot_general(a, b, dims, preferred_element_type=F32)


def grid2(rows, cols):
    return (
        lax.broadcasted_iota(jnp.int32, (rows, cols), 0),
        lax.broadcasted_iota(jnp.int32, (rows, cols), 1),
    )


def one_hot(cond):
    return jnp.where(cond, 1.0, 0.0).astype(BF16)


def stack_matrix(re, im):
    upper = jnp.concatenate([re, -im], 1)
    lower = jnp.concatenate([im, re], 1)
    return jnp.concatenate([upper, lower], 0)


def coefficients(idx_ref, term_ref, path, even):
    term = idx_ref[path]
    pick = lambda c, m, j: term_ref[c, m, j, term]
    spread = lambda s0, s1: jnp.where(even, s0, s1)
    return (
        spread(pick(0, 0, 0), pick(0, 1, 1)),
        spread(pick(1, 0, 0), pick(1, 1, 1)),
        spread(pick(0, 0, 1), pick(0, 1, 0)),
        spread(pick(1, 0, 1), pick(1, 1, 0)),
    )


def cut_paths(slab, first_path, idx_ref, term_ref, pair_swap, even):
    paths, _, rows, width = slab.shape
    flat = slab.reshape(paths * 2 * rows, width)
    swapped = dot(flat, pair_swap)
    wide = flat.astype(F32)
    done = []
    for p in range(paths):
        at = 2 * p * rows
        xr, xi = wide[at : at + rows], wide[at + rows : at + 2 * rows]
        sr, si = swapped[at : at + rows], swapped[at + rows : at + 2 * rows]
        ar, ai, br, bi = coefficients(idx_ref, term_ref, first_path + p, even)
        cr = (xr * ar + sr * br) - (xi * ai + si * bi)
        ci = (xr * ai + sr * bi) + (xi * ar + si * br)
        done.append(jnp.concatenate([cr, ci], 1).astype(BF16))
    return jnp.concatenate(done, 0)


def exchange_kernel(
    chips,
    idx_hbm, lterm_hbm, rterm_hbm,
    left_ref, right_ref, lgate_hbm, rgate_hbm,
    total_ref, last_ref, lhs_ref,
    idx_ref, lterm_ref, rterm_ref, lgate_ref, rgate_ref,
    lx, rx, lt, rt, lsend, early, up, down, peer_blocks, own_blocks, lhs_now,
    in_sem, swap_send, swap_recv,
    ag_send, ag_recv, aa_send, aa_recv, pr_send, pr_recv,
):
    me = lax.axis_index("path")
    core = lax.axis_index("amp")
    nxt, prv = lax.rem(me + 1, chips), lax.rem(me + chips - 1, chips)
    peer = {"amp": 1 - core}
    toward = ({"path": nxt}, {"path": prv})
    half = chips // 2
    pieces, wide = early.shape[1], early.shape[3]
    held = early.shape[0]

    barrier = pltpu.get_barrier_semaphore()
    for who in (peer, *toward):
        pl.semaphore_signal(barrier, inc=1, device_id=who, device_id_type=MESH)
    loads = [
        pltpu.make_async_copy(src, dst, in_sem.at[n])
        for n, (src, dst) in enumerate((
            (rgate_hbm, rgate_ref), (idx_hbm, idx_ref), (rterm_hbm, rterm_ref),
            (lterm_hbm, lterm_ref), (lgate_hbm, lgate_ref)))
    ]
    for load in loads:
        load.start()
    pl.semaphore_wait(barrier, 3)

    mine = lx.shape[0]
    lrows, rrows = left_ref.shape[2], right_ref.shape[2]
    rplace = pl.ds(pl.multiple_of(core * rrows, rrows), rrows)
    lplace = pl.ds(pl.multiple_of(core * lrows, lrows), lrows)
    give_right = pltpu.make_async_remote_copy(
        src_ref=right_ref, dst_ref=rx.at[:, :, rplace],
        send_sem=swap_send.at[0], recv_sem=swap_recv.at[0], device_id=peer, device_id_type=MESH)
    give_left = pltpu.make_async_remote_copy(
        src_ref=left_ref.at[pl.ds((1 - core) * mine, mine)], dst_ref=lx.at[:, :, lplace],
        send_sem=swap_send.at[1], recv_sem=swap_recv.at[1], device_id=peer, device_id_type=MESH)
    give_right.start()
    give_left.start()
    rx[:, :, rplace] = right_ref[...]
    lx[:, :, lplace] = left_ref[pl.ds(core * mine, mine)]

    for load in loads[:3]:
        load.wait()
    row, col = grid2(128, 128)
    pair_swap = one_hot(row == (col ^ 1))
    even = (lax.broadcasted_iota(jnp.int32, (1, 128), 1) & 1) == 0
    prow, pcol = grid2(256, 256)
    regroup = one_hot(pcol == (prow % 8) * 32 + prow // 8)

    s_low = stack_matrix(rgate_ref[0, 0], rgate_ref[0, 1])
    s_low = jnp.concatenate(
        [s_low, s_low[64:128], s_low[0:64], s_low[192:256], s_low[128:192]], 0)
    here = rrows
    full = 2 * here
    srow, scol = grid2(here, 128)
    krow, kcol = grid2(2 * full, 128)
    parts = []
    for c in range(2):
        gate = rgate_ref[1, c]
        rows_of = []
        for t in range(2):
            pick_rows = one_hot(scol == 2 * (core * here + srow) + t)
            pick_cols = one_hot(kcol == 2 * (krow % full) + (krow // full + t) % 2)
            some = dot(pick_rows, gate).astype(BF16)
            rows_of.append(dot(some, pick_cols, NT).astype(BF16))
        parts.append(jnp.concatenate(rows_of, 0))
    s_high = stack_matrix(parts[0], parts[1])

    give_right.wait_recv()
    low_lanes = lax.broadcasted_iota(jnp.int32, (1, 128), 1) < 64
    step = 4
    for first in range(0, rx.shape[0], step):
        cut = cut_paths(rx[first : first + step], first, idx_ref, rterm_ref, pair_swap, even)
        low = dot(cut, s_low, NT).astype(BF16)
        tall = []
        for p in range(step):
            at = low[p * full : (p + 1) * full]
            tall.append(jnp.concatenate(
                [at[:, 0:128], at[:, 256:384], at[:, 128:256], at[:, 384:512]], 0))
        turned = dot(s_high, jnp.concatenate(tall, 1))
        for p in range(step):
            z = turned[:, p * 128 : (p + 1) * 128]
            q = first + p
            for c in range(2):
                at = 2 * c * here
                pair = jnp.where(low_lanes, z[at : at + here], z[at + here : at + 2 * here])
                rt[c, q // 8, (q % 8) * 32 : (q % 8) * 32 + here] = pair.astype(BF16)
    per_piece = here // pieces
    for g in range(2):
        both = [dot(regroup, rt[c, g]) for c in range(2)]
        for r in range(here):
            tile = jnp.concatenate([b[r * 8 : r * 8 + 8] for b in both], 0).astype(BF16)
            at = (r % per_piece) * 128
            early[0, r // per_piece, g * 16 : g * 16 + 16, at : at + 128] = tile

    def slot_of(d, s):
        return min(2 * s - (1 - d), chips - 1) if s else 0

    def right_slot(n):
        return early.at[n] if n < held else last_ref.at[n - held]

    def gather_copy(d, s, j):
        return pltpu.make_async_remote_copy(
            src_ref=right_slot(slot_of(d, s)).at[j], dst_ref=right_slot(slot_of(d, s + 1)).at[j],
            send_sem=ag_send.at[d, s, j], recv_sem=ag_recv.at[d, s, j],
            device_id=toward[d], device_id_type=MESH)

    gather_steps = (half - 1, half)
    group = chips // 4
    slice_cols = wide // pieces

    def add_slice(g, piece, j):
        at = pl.ds(pl.multiple_of(j * slice_cols, slice_cols), slice_cols)
        right = early[g * group : (g + 1) * group, piece, :, at].reshape(-1, slice_cols)
        to = pl.ds(pl.multiple_of(piece * wide + j * slice_cols, slice_cols), slice_cols)
        more = dot(lhs_now[...], right)
        total_ref[:, to] = more if g == 0 else total_ref[:, to] + more

    def gather_step(s, work=None):
        @pl.loop(0, pieces)
        def _(j):
            for d in range(2):
                if 1 <= s <= gather_steps[d]:
                    gather_copy(d, s - 1, j).wait_recv()
                if s < gather_steps[d]:
                    gather_copy(d, s, j).start()
            if work is not None:
                add_slice(*work, j)

    gather_step(0)
    for load in loads[3:]:
        load.wait()

    s_low = stack_matrix(lgate_ref[0, 0], lgate_ref[0, 1])
    s_high = stack_matrix(lgate_ref[1, 0], lgate_ref[1, 1])
    give_left.wait_recv()
    step = 2
    groups = 4
    for first in range(0, mine, step):
        cut = cut_paths(
            lx[first : first + step], core * mine + first, idx_ref, lterm_ref, pair_swap, even)
        low = dot(cut, s_low, NT).astype(BF16)
        tall = [
            jnp.concatenate([low[p * 128 : (p + 1) * 128, c * 128 : (c + 1) * 128] for c in range(2)], 0)
            for p in range(step)
        ]
        turned = dot(s_high, jnp.concatenate(tall, 1)).astype(BF16)
        for p in range(step):
            for c in range(2):
                for g in range(groups):
                    at = c * 128 + g * 32
                    lt[c, g, (first + p) * 32 : (first + p) * 32 + 32] = (
                        turned[at : at + 32, p * 128 : (p + 1) * 128])
    per_chip = 128 // chips
    for g in range(groups):
        both = [dot(regroup, lt[c, g]) for c in range(2)]
        for r in range(32):
            m = g * 32 + r
            tile = jnp.concatenate([b[r * 8 : r * 8 + 8] for b in both], 0).astype(BF16)
            slot = lax.rem(m // per_chip - me + chips, chips)
            at = (m % per_chip) * 128
            lsend[slot, :, at : at + 128] = tile

    counts = ([half - s for s in range(half)], [half - 1 - s for s in range(half - 1)])
    bases = [[sum(c[:s]) for s in range(len(c))] for c in counts]
    landing = (up, down)

    def block_copy(d, s):
        n = counts[d][s]
        if s == 0:
            src = lsend.at[pl.ds(1, n)] if d == 0 else lsend.at[pl.ds(half + 1, n)]
        else:
            src = landing[d].at[pl.ds(bases[d][s - 1] + (1 if d == 0 else 0), n)]
        return pltpu.make_async_remote_copy(
            src_ref=src, dst_ref=landing[d].at[pl.ds(bases[d][s], n)],
            send_sem=aa_send.at[d, s], recv_sem=aa_recv.at[d, s],
            device_id=toward[d], device_id_type=MESH)

    handed = []

    def hand_over(src, n):
        there = pltpu.make_async_remote_copy(
            src_ref=src, dst_ref=peer_blocks.at[n],
            send_sem=pr_send.at[n], recv_sem=pr_recv.at[n], device_id=peer, device_id_type=MESH)
        there.start()
        handed.append((n, there))
        own_blocks[n] = src[...]

    def block_step(s):
        for d in range(2):
            if 1 <= s <= len(counts[d]):
                block_copy(d, s - 1).wait_recv()
            if s < len(counts[d]):
                block_copy(d, s).start()
            if s == 0 and d == 0:
                hand_over(lsend.at[0], 0)
            if 1 <= s <= len(counts[d]):
                at = bases[d][s - 1] + (0 if d == 0 else counts[d][s - 1] - 1)
                hand_over(landing[d].at[at], slot_of(d, s) if s < half else chips - 1)

    krow, kcol = grid2(16 * 2 * group, 16 * 2 * group)
    imag = (krow // 8) % 2 == 1
    signed = jnp.where(krow == kcol, jnp.where(imag, -1.0, 1.0), 0.0).astype(BF16)
    crossed = one_hot(krow == (kcol ^ 8))

    def build_lhs(g, to_ref):
        rows = []
        for n in range(g * group, (g + 1) * group):
            dict(handed)[n].wait_recv()
            own, other = own_blocks[n], peer_blocks[n]
            first = core == 0
            rows.append(jnp.where(first, own, other))
            rows.append(jnp.where(first, other, own))
        block = jnp.concatenate(rows, 0)
        to_ref[0 : block.shape[1]] = dot(block, signed, TN).astype(BF16)
        to_ref[block.shape[1] :] = dot(block, crossed, TN).astype(BF16)

    block_step(0)
    quarter = half // 4
    for s in range(1, half + 1):
        ready, phase = divmod(s - 1, quarter)
        if s == half:
            block_step(s)
            build_lhs(3, lhs_ref)
        if phase == 0 and ready >= 1:
            build_lhs(ready - 1, lhs_now)
        gather_step(s, (ready - 1, phase) if ready >= 1 else None)
        if s < half:
            block_step(s)

    give_right.wait_send()
    give_left.wait_send()
    for s in range(half):
        @pl.loop(0, pieces)
        def _(j):
            for d in range(2):
                if s < gather_steps[d]:
                    gather_copy(d, s, j).wait_send()
        for d in range(2):
            if s < len(counts[d]):
                block_copy(d, s).wait_send()
    for _, there in handed:
        there.wait_send()


def finish_kernel(total_ref, last_ref, lhs_ref, out_ref, staged, sems):
    count, _, rows, tile = staged.shape
    per = last_ref.shape[3] // tile

    def put(k):
        to = pl.ds(pl.multiple_of(k * tile, tile), tile)
        return pltpu.make_async_copy(staged.at[k], out_ref.at[:, :, to], sems.at[k])

    @pl.loop(0, count)
    def _(k):
        at = pl.ds(pl.multiple_of(lax.rem(k, per) * tile, tile), tile)
        right = last_ref[:, k // per, :, at].reshape(-1, tile)
        to = pl.ds(pl.multiple_of(k * tile, tile), tile)
        for c in range(2):
            part = slice(c * rows, (c + 1) * rows)
            staged[k, c] = (total_ref[part, to] + dot(lhs_ref[part], right)).astype(BF16)
        put(k).start()

    @pl.loop(0, count)
    def _(k):
        put(k).wait()


def shards(left_slabs, right_slabs, term_index, left_terms, right_terms, left_gates, right_gates):
    chips = lax.axis_size("path")
    paths = left_slabs.shape[0]
    mine = paths // 2
    left = left_slabs.reshape(paths, 2, -1, 128)
    right = right_slabs.reshape(paths, 2, -1, 128)
    lrows, rrows = left.shape[2], right.shape[2]
    half = chips // 2
    pieces = half // 4
    cols = rrows * 128
    block = 2 * lrows * 128 // chips
    vmem = pl.BlockSpec(memory_space=pltpu.VMEM)
    hbm = pl.BlockSpec(memory_space=pltpu.HBM)
    dma = pltpu.SemaphoreType.DMA
    held = chips // 4 * 3
    wide = cols // pieces
    depth = chips // 4 * 2 * paths
    blocks = (2 * mine, block)
    total, last, lhs = pl.pallas_call(
        functools.partial(exchange_kernel, chips),
        out_shape=(
            jax.ShapeDtypeStruct((2 * block, cols), F32),
            jax.ShapeDtypeStruct((chips - held, pieces, 2 * paths, wide), BF16),
            jax.ShapeDtypeStruct((2 * block, depth), BF16),
        ),
        in_specs=[hbm, hbm, hbm, vmem, vmem, hbm, hbm],
        out_specs=(vmem, vmem, vmem),
        scratch_shapes=[
            pltpu.SMEM((paths,), jnp.int32),
            pltpu.SMEM((2, 2, 2, 4), F32),
            pltpu.SMEM((2, 2, 2, 4), F32),
            pltpu.VMEM(left_gates.shape, BF16),
            pltpu.VMEM(right_gates.shape, BF16),
            pltpu.VMEM((mine, 2, 2 * lrows, 128), BF16),
            pltpu.VMEM((paths, 2, 2 * rrows, 128), BF16),
            pltpu.VMEM((2, 4, 256, 128), BF16),
            pltpu.VMEM((2, 2, 256, 128), BF16),
            pltpu.VMEM((chips, *blocks), BF16),
            pltpu.VMEM((held, pieces, 2 * paths, wide), BF16),
            pltpu.VMEM((half * (half + 1) // 2, *blocks), BF16),
            pltpu.VMEM((half * (half - 1) // 2, *blocks), BF16),
            pltpu.VMEM((chips, *blocks), BF16),
            pltpu.VMEM((chips, *blocks), BF16),
            pltpu.VMEM((2 * block, depth), BF16),
            dma((5,)), dma((2,)), dma((2,)),
            dma((2, half, pieces)), dma((2, half, pieces)),
            dma((2, half)), dma((2, half)),
            dma((chips,)), dma((chips,)),
        ],
        compiler_params=pltpu.CompilerParams(
            collective_id=0, has_side_effects=True, vmem_limit_bytes=VMEM_LIMIT),
        name="exchange",
    )(
        *(pltpu.with_memory_space_constraint(x, pltpu.HBM) for x in (
            term_index, jnp.transpose(left_terms, (1, 2, 3, 0)), jnp.transpose(right_terms, (1, 2, 3, 0)))),
        left, right,
        *(pltpu.with_memory_space_constraint(x, pltpu.HBM) for x in (left_gates, right_gates)),
    )
    tile = min(512, wide)
    return pl.pallas_call(
        finish_kernel,
        out_shape=jax.ShapeDtypeStruct((2, block, cols), BF16),
        in_specs=[vmem, vmem, vmem],
        out_specs=hbm,
        scratch_shapes=[
            pltpu.VMEM((cols // tile, 2, block, tile), BF16),
            pltpu.SemaphoreType.DMA((cols // tile,)),
        ],
        compiler_params=pltpu.CompilerParams(vmem_limit_bytes=16 * 1024 * 1024),
        name="finish",
    )(total, last, lhs)


def solution(mesh):
    return jax.shard_map(
        shards,
        mesh=mesh,
        in_specs=(
            P(("grp", "path"), None, "amp"),
            P(("grp", "path"), None, "amp"),
            P(("grp", "path")),
            P(),
            P(),
            P(),
            P(),
        ),
        out_specs=P(None, ("grp", "path"), "amp"),
        check_vma=False,
    )
```

```python
import functools

import jax
import jax.numpy as jnp
from jax import lax
from jax.experimental import pallas as pl
from jax.experimental.pallas import tpu as pltpu
from jax.sharding import PartitionSpec as P

MESH = pl.DeviceIdType.MESH
F32 = jnp.float32
BF16 = jnp.bfloat16
VMEM_LIMIT = 24 * 1024 * 1024
NT = (((1,), (1,)), ((), ()))
TN = (((0,), (0,)), ((), ()))


def dot(a, b, dims=(((1,), (0,)), ((), ()))):
    return lax.dot_general(a, b, dims, preferred_element_type=F32)


def grid2(rows, cols):
    return (
        lax.broadcasted_iota(jnp.int32, (rows, cols), 0),
        lax.broadcasted_iota(jnp.int32, (rows, cols), 1),
    )


def one_hot(cond):
    return jnp.where(cond, 1.0, 0.0).astype(BF16)


def stack_matrix(re, im):
    upper = jnp.concatenate([re, -im], 1)
    lower = jnp.concatenate([im, re], 1)
    return jnp.concatenate([upper, lower], 0)


def coefficients(idx_ref, term_ref, path, even):
    term = idx_ref[path]
    pick = lambda c, m, j: term_ref[c, m, j, term]
    spread = lambda s0, s1: jnp.where(even, s0, s1)
    return (
        spread(pick(0, 0, 0), pick(0, 1, 1)),
        spread(pick(1, 0, 0), pick(1, 1, 1)),
        spread(pick(0, 0, 1), pick(0, 1, 0)),
        spread(pick(1, 0, 1), pick(1, 1, 0)),
    )


def cut_paths(slab, first_path, idx_ref, term_ref, pair_swap, even):
    paths, _, rows, width = slab.shape
    flat = slab.reshape(paths * 2 * rows, width)
    swapped = dot(flat, pair_swap)
    wide = flat.astype(F32)
    done = []
    for p in range(paths):
        at = 2 * p * rows
        xr, xi = wide[at : at + rows], wide[at + rows : at + 2 * rows]
        sr, si = swapped[at : at + rows], swapped[at + rows : at + 2 * rows]
        ar, ai, br, bi = coefficients(idx_ref, term_ref, first_path + p, even)
        cr = (xr * ar + sr * br) - (xi * ai + si * bi)
        ci = (xr * ai + sr * bi) + (xi * ar + si * br)
        done.append(jnp.concatenate([cr, ci], 1).astype(BF16))
    return jnp.concatenate(done, 0)


def exchange_kernel(
    chips,
    idx_hbm, lterm_hbm, rterm_hbm,
    left_hbm, right_hbm, lgate_hbm, rgate_hbm,
    total_ref, last_ref, lhs_ref,
    idx_ref, lterm_ref, rterm_ref, lgate_ref, rgate_ref,
    lraw, rraw, lx, rx, lt, rt, lsend, early, up, down, peer_blocks, own_blocks, lhs_now,
    in_sem, swap_send, swap_recv,
    ag_send, ag_recv, aa_send, aa_recv, pr_send, pr_recv,
):
    me = lax.axis_index("path")
    core = lax.axis_index("amp")
    nxt, prv = lax.rem(me + 1, chips), lax.rem(me + chips - 1, chips)
    peer = {"amp": 1 - core}
    toward = ({"path": nxt}, {"path": prv})
    half = chips // 2
    pieces, wide = early.shape[1], early.shape[3]
    held = early.shape[0]

    barrier = pltpu.get_barrier_semaphore()
    for who in (peer, *toward):
        pl.semaphore_signal(barrier, inc=1, device_id=who, device_id_type=MESH)
    mine = lx.shape[0]
    loads = [
        pltpu.make_async_copy(src, dst, in_sem.at[n])
        for n, (src, dst) in enumerate((
            (right_hbm, rraw.at[:, core]),
            (rgate_hbm, rgate_ref), (idx_hbm, idx_ref), (rterm_hbm, rterm_ref),
            (lterm_hbm, lterm_ref), (lgate_hbm, lgate_ref),
            (left_hbm.at[pl.ds(core * mine, mine)], lraw.at[:, core])))
    ]
    for load in loads:
        load.start()
    pl.semaphore_wait(barrier, 3)

    rrows, lrows = rx.shape[2] // 2, lx.shape[2] // 2
    give_right = pltpu.make_async_remote_copy(
        src_ref=right_hbm, dst_ref=rraw.at[:, core],
        send_sem=swap_send.at[0], recv_sem=swap_recv.at[0], device_id=peer, device_id_type=MESH)
    give_left = pltpu.make_async_remote_copy(
        src_ref=left_hbm.at[pl.ds((1 - core) * mine, mine)], dst_ref=lraw.at[:, core],
        send_sem=swap_send.at[1], recv_sem=swap_recv.at[1], device_id=peer, device_id_type=MESH)
    give_right.start()
    give_left.start()

    def to_rows(raw, full, part, count):
        @pl.loop(0, raw.shape[0], unroll=4)
        def _(p):
            at = pl.ds(pl.multiple_of(part * count, count), count)
            full[p, :, at] = raw[p, part].reshape(2, count, 128)

    loads[0].wait()
    to_rows(rraw, rx, core, rrows)
    for load in loads[1:4]:
        load.wait()
    row, col = grid2(128, 128)
    pair_swap = one_hot(row == (col ^ 1))
    even = (lax.broadcasted_iota(jnp.int32, (1, 128), 1) & 1) == 0
    prow, pcol = grid2(256, 256)
    regroup = one_hot(pcol == (prow % 8) * 32 + prow // 8)

    s_low = stack_matrix(rgate_ref[0, 0], rgate_ref[0, 1])
    s_low = jnp.concatenate(
        [s_low, s_low[64:128], s_low[0:64], s_low[192:256], s_low[128:192]], 0)
    here = rrows
    full = 2 * here
    srow, scol = grid2(here, 128)
    krow, kcol = grid2(2 * full, 128)
    parts = []
    for c in range(2):
        gate = rgate_ref[1, c]
        rows_of = []
        for t in range(2):
            pick_rows = one_hot(scol == 2 * (core * here + srow) + t)
            pick_cols = one_hot(kcol == 2 * (krow % full) + (krow // full + t) % 2)
            some = dot(pick_rows, gate).astype(BF16)
            rows_of.append(dot(some, pick_cols, NT).astype(BF16))
        parts.append(jnp.concatenate(rows_of, 0))
    s_high = stack_matrix(parts[0], parts[1])

    give_right.wait_recv()
    to_rows(rraw, rx, 1 - core, rrows)
    low_lanes = lax.broadcasted_iota(jnp.int32, (1, 128), 1) < 64
    step = 4
    for first in range(0, rx.shape[0], step):
        cut = cut_paths(rx[first : first + step], first, idx_ref, rterm_ref, pair_swap, even)
        low = dot(cut, s_low, NT).astype(BF16)
        tall = []
        for p in range(step):
            at = low[p * full : (p + 1) * full]
            tall.append(jnp.concatenate(
                [at[:, 0:128], at[:, 256:384], at[:, 128:256], at[:, 384:512]], 0))
        turned = dot(s_high, jnp.concatenate(tall, 1))
        for p in range(step):
            z = turned[:, p * 128 : (p + 1) * 128]
            q = first + p
            for c in range(2):
                at = 2 * c * here
                pair = jnp.where(low_lanes, z[at : at + here], z[at + here : at + 2 * here])
                rt[c, q // 8, (q % 8) * 32 : (q % 8) * 32 + here] = pair.astype(BF16)
    per_piece = here // pieces
    for g in range(2):
        both = [dot(regroup, rt[c, g]) for c in range(2)]
        for r in range(here):
            tile = jnp.concatenate([b[r * 8 : r * 8 + 8] for b in both], 0).astype(BF16)
            at = (r % per_piece) * 128
            early[0, r // per_piece, g * 16 : g * 16 + 16, at : at + 128] = tile

    def slot_of(d, s):
        return min(2 * s - (1 - d), chips - 1) if s else 0

    def right_slot(n):
        return early.at[n] if n < held else last_ref.at[n - held]

    def gather_copy(d, s, j):
        return pltpu.make_async_remote_copy(
            src_ref=right_slot(slot_of(d, s)).at[j], dst_ref=right_slot(slot_of(d, s + 1)).at[j],
            send_sem=ag_send.at[d, s, j], recv_sem=ag_recv.at[d, s, j],
            device_id=toward[d], device_id_type=MESH)

    gather_steps = (half - 1, half)
    group = chips // 4
    slice_cols = wide // pieces

    def add_slice(g, piece, j):
        at = pl.ds(pl.multiple_of(j * slice_cols, slice_cols), slice_cols)
        right = early[g * group : (g + 1) * group, piece, :, at].reshape(-1, slice_cols)
        to = pl.ds(pl.multiple_of(piece * wide + j * slice_cols, slice_cols), slice_cols)
        more = dot(lhs_now[...], right)
        total_ref[:, to] = more if g == 0 else total_ref[:, to] + more

    def gather_step(s, work=None):
        @pl.loop(0, pieces)
        def _(j):
            for d in range(2):
                if 1 <= s <= gather_steps[d]:
                    gather_copy(d, s - 1, j).wait_recv()
                if s < gather_steps[d]:
                    gather_copy(d, s, j).start()
            if work is not None:
                add_slice(*work, j)

    gather_step(0)
    for load in loads[4:]:
        load.wait()

    s_low = stack_matrix(lgate_ref[0, 0], lgate_ref[0, 1])
    s_high = stack_matrix(lgate_ref[1, 0], lgate_ref[1, 1])
    give_left.wait_recv()
    for part in range(2):
        to_rows(lraw, lx, part, lrows)
    step = 2
    groups = 4
    for first in range(0, mine, step):
        cut = cut_paths(
            lx[first : first + step], core * mine + first, idx_ref, lterm_ref, pair_swap, even)
        low = dot(cut, s_low, NT).astype(BF16)
        tall = [
            jnp.concatenate([low[p * 128 : (p + 1) * 128, c * 128 : (c + 1) * 128] for c in range(2)], 0)
            for p in range(step)
        ]
        turned = dot(s_high, jnp.concatenate(tall, 1)).astype(BF16)
        for p in range(step):
            for c in range(2):
                for g in range(groups):
                    at = c * 128 + g * 32
                    lt[c, g, (first + p) * 32 : (first + p) * 32 + 32] = (
                        turned[at : at + 32, p * 128 : (p + 1) * 128])
    per_chip = 128 // chips
    for g in range(groups):
        both = [dot(regroup, lt[c, g]) for c in range(2)]
        for r in range(32):
            m = g * 32 + r
            tile = jnp.concatenate([b[r * 8 : r * 8 + 8] for b in both], 0).astype(BF16)
            slot = lax.rem(m // per_chip - me + chips, chips)
            at = (m % per_chip) * 128
            lsend[slot, :, at : at + 128] = tile

    counts = ([half - s for s in range(half)], [half - 1 - s for s in range(half - 1)])
    bases = [[sum(c[:s]) for s in range(len(c))] for c in counts]
    landing = (up, down)

    def block_copy(d, s):
        n = counts[d][s]
        if s == 0:
            src = lsend.at[pl.ds(1, n)] if d == 0 else lsend.at[pl.ds(half + 1, n)]
        else:
            src = landing[d].at[pl.ds(bases[d][s - 1] + (1 if d == 0 else 0), n)]
        return pltpu.make_async_remote_copy(
            src_ref=src, dst_ref=landing[d].at[pl.ds(bases[d][s], n)],
            send_sem=aa_send.at[d, s], recv_sem=aa_recv.at[d, s],
            device_id=toward[d], device_id_type=MESH)

    handed = []

    def hand_over(src, n):
        there = pltpu.make_async_remote_copy(
            src_ref=src, dst_ref=peer_blocks.at[n],
            send_sem=pr_send.at[n], recv_sem=pr_recv.at[n], device_id=peer, device_id_type=MESH)
        there.start()
        handed.append((n, there))
        own_blocks[n] = src[...]

    def block_step(s):
        for d in range(2):
            if 1 <= s <= len(counts[d]):
                block_copy(d, s - 1).wait_recv()
            if s < len(counts[d]):
                block_copy(d, s).start()
            if s == 0 and d == 0:
                hand_over(lsend.at[0], 0)
            if 1 <= s <= len(counts[d]):
                at = bases[d][s - 1] + (0 if d == 0 else counts[d][s - 1] - 1)
                hand_over(landing[d].at[at], slot_of(d, s) if s < half else chips - 1)

    krow, kcol = grid2(16 * 2 * group, 16 * 2 * group)
    imag = (krow // 8) % 2 == 1
    signed = jnp.where(krow == kcol, jnp.where(imag, -1.0, 1.0), 0.0).astype(BF16)
    crossed = one_hot(krow == (kcol ^ 8))

    def build_lhs(g, to_ref):
        rows = []
        for n in range(g * group, (g + 1) * group):
            dict(handed)[n].wait_recv()
            own, other = own_blocks[n], peer_blocks[n]
            first = core == 0
            rows.append(jnp.where(first, own, other))
            rows.append(jnp.where(first, other, own))
        block = jnp.concatenate(rows, 0)
        to_ref[0 : block.shape[1]] = dot(block, signed, TN).astype(BF16)
        to_ref[block.shape[1] :] = dot(block, crossed, TN).astype(BF16)

    block_step(0)
    quarter = half // 4
    for s in range(1, half + 1):
        ready, phase = divmod(s - 1, quarter)
        if s == half:
            block_step(s)
            build_lhs(3, lhs_ref)
        if phase == 0 and ready >= 1:
            build_lhs(ready - 1, lhs_now)
        gather_step(s, (ready - 1, phase) if ready >= 1 else None)
        if s < half:
            block_step(s)

    give_right.wait_send()
    give_left.wait_send()
    for s in range(half):
        @pl.loop(0, pieces)
        def _(j):
            for d in range(2):
                if s < gather_steps[d]:
                    gather_copy(d, s, j).wait_send()
        for d in range(2):
            if s < len(counts[d]):
                block_copy(d, s).wait_send()
    for _, there in handed:
        there.wait_send()


def finish_kernel(total_ref, last_ref, lhs_ref, out_ref, staged, sems):
    count, _, rows, tile = staged.shape
    per = last_ref.shape[3] // tile

    def put(k):
        to = pl.ds(pl.multiple_of(k * tile, tile), tile)
        return pltpu.make_async_copy(staged.at[k], out_ref.at[:, :, to], sems.at[k])

    @pl.loop(0, count)
    def _(k):
        at = pl.ds(pl.multiple_of(lax.rem(k, per) * tile, tile), tile)
        right = last_ref[:, k // per, :, at].reshape(-1, tile)
        to = pl.ds(pl.multiple_of(k * tile, tile), tile)
        for c in range(2):
            part = slice(c * rows, (c + 1) * rows)
            staged[k, c] = (total_ref[part, to] + dot(lhs_ref[part], right)).astype(BF16)
        put(k).start()

    @pl.loop(0, count)
    def _(k):
        put(k).wait()


def shards(left_slabs, right_slabs, term_index, left_terms, right_terms, left_gates, right_gates):
    chips = lax.axis_size("path")
    paths = left_slabs.shape[0]
    mine = paths // 2
    lrows, rrows = left_slabs.shape[2] // 128, right_slabs.shape[2] // 128
    half = chips // 2
    pieces = half // 4
    cols = rrows * 128
    block = 2 * lrows * 128 // chips
    vmem = pl.BlockSpec(memory_space=pltpu.VMEM)
    hbm = pl.BlockSpec(memory_space=pltpu.HBM)
    dma = pltpu.SemaphoreType.DMA
    held = chips // 4 * 3
    wide = cols // pieces
    depth = chips // 4 * 2 * paths
    blocks = (2 * mine, block)
    total, last, lhs = pl.pallas_call(
        functools.partial(exchange_kernel, chips),
        out_shape=(
            jax.ShapeDtypeStruct((2 * block, cols), F32),
            jax.ShapeDtypeStruct((chips - held, pieces, 2 * paths, wide), BF16),
            jax.ShapeDtypeStruct((2 * block, depth), BF16),
        ),
        in_specs=[hbm] * 7,
        out_specs=(vmem, vmem, vmem),
        scratch_shapes=[
            pltpu.SMEM((paths,), jnp.int32),
            pltpu.SMEM((2, 2, 2, 4), F32),
            pltpu.SMEM((2, 2, 2, 4), F32),
            pltpu.VMEM(left_gates.shape, BF16),
            pltpu.VMEM(right_gates.shape, BF16),
            pltpu.VMEM((mine, 2, 2, lrows * 128), BF16),
            pltpu.VMEM((paths, 2, 2, rrows * 128), BF16),
            pltpu.VMEM((mine, 2, 2 * lrows, 128), BF16),
            pltpu.VMEM((paths, 2, 2 * rrows, 128), BF16),
            pltpu.VMEM((2, 4, 256, 128), BF16),
            pltpu.VMEM((2, 2, 256, 128), BF16),
            pltpu.VMEM((chips, *blocks), BF16),
            pltpu.VMEM((held, pieces, 2 * paths, wide), BF16),
            pltpu.VMEM((half * (half + 1) // 2, *blocks), BF16),
            pltpu.VMEM((half * (half - 1) // 2, *blocks), BF16),
            pltpu.VMEM((chips, *blocks), BF16),
            pltpu.VMEM((chips, *blocks), BF16),
            pltpu.VMEM((2 * block, depth), BF16),
            dma((7,)), dma((2,)), dma((2,)),
            dma((2, half, pieces)), dma((2, half, pieces)),
            dma((2, half)), dma((2, half)),
            dma((chips,)), dma((chips,)),
        ],
        compiler_params=pltpu.CompilerParams(
            collective_id=0, has_side_effects=True, vmem_limit_bytes=VMEM_LIMIT),
        name="exchange",
    )(
        *(pltpu.with_memory_space_constraint(x, pltpu.HBM) for x in (
            term_index, jnp.transpose(left_terms, (1, 2, 3, 0)), jnp.transpose(right_terms, (1, 2, 3, 0)),
            left_slabs, right_slabs, left_gates, right_gates)),
    )
    tile = min(512, wide)
    return pl.pallas_call(
        finish_kernel,
        out_shape=jax.ShapeDtypeStruct((2, block, cols), BF16),
        in_specs=[vmem, vmem, vmem],
        out_specs=hbm,
        scratch_shapes=[
            pltpu.VMEM((cols // tile, 2, block, tile), BF16),
            pltpu.SemaphoreType.DMA((cols // tile,)),
        ],
        compiler_params=pltpu.CompilerParams(vmem_limit_bytes=16 * 1024 * 1024),
        name="finish",
    )(total, last, lhs)


def solution(mesh):
    return jax.shard_map(
        shards,
        mesh=mesh,
        in_specs=(
            P(("grp", "path"), None, "amp"),
            P(("grp", "path"), None, "amp"),
            P(("grp", "path")),
            P(),
            P(),
            P(),
            P(),
        ),
        out_specs=P(None, ("grp", "path"), "amp"),
        check_vma=False,
    )
```

```python
import functools

import jax
import jax.numpy as jnp
from jax import lax
from jax.experimental import pallas as pl
from jax.experimental.pallas import tpu as pltpu
from jax.sharding import PartitionSpec as P

MESH = pl.DeviceIdType.MESH
F32 = jnp.float32
BF16 = jnp.bfloat16
PIECES = 4
VMEM_LIMIT = 24 * 1024 * 1024
NT = (((1,), (1,)), ((), ()))
TN = (((0,), (0,)), ((), ()))


def dot(a, b, dims=(((1,), (0,)), ((), ()))):
    return lax.dot_general(a, b, dims, preferred_element_type=F32)


def grid2(rows, cols):
    return (
        lax.broadcasted_iota(jnp.int32, (rows, cols), 0),
        lax.broadcasted_iota(jnp.int32, (rows, cols), 1),
    )


def one_hot(cond):
    return jnp.where(cond, 1.0, 0.0).astype(BF16)


def stack_matrix(re, im):
    upper = jnp.concatenate([re, -im], 1)
    lower = jnp.concatenate([im, re], 1)
    return jnp.concatenate([upper, lower], 0)


def coefficients(idx_ref, term_ref, path, even):
    term = idx_ref[path]
    pick = lambda c, m, j: term_ref[c, m, j, term]
    spread = lambda s0, s1: jnp.where(even, s0, s1)
    return (
        spread(pick(0, 0, 0), pick(0, 1, 1)),
        spread(pick(1, 0, 0), pick(1, 1, 1)),
        spread(pick(0, 0, 1), pick(0, 1, 0)),
        spread(pick(1, 0, 1), pick(1, 1, 0)),
    )


def cut_paths(slab, first_path, idx_ref, term_ref, pair_swap, even):
    paths, _, rows, width = slab.shape
    flat = slab.reshape(paths * 2 * rows, width)
    swapped = dot(flat, pair_swap)
    wide = flat.astype(F32)
    done = []
    for p in range(paths):
        at = 2 * p * rows
        xr, xi = wide[at : at + rows], wide[at + rows : at + 2 * rows]
        sr, si = swapped[at : at + rows], swapped[at + rows : at + 2 * rows]
        ar, ai, br, bi = coefficients(idx_ref, term_ref, first_path + p, even)
        cr = (xr * ar + sr * br) - (xi * ai + si * bi)
        ci = (xr * ai + sr * bi) + (xi * ar + si * br)
        done.append(jnp.concatenate([cr, ci], 1).astype(BF16))
    return jnp.concatenate(done, 0)


def exchange_kernel(
    chips,
    idx_hbm, lterm_hbm, rterm_hbm,
    left_hbm, right_hbm, lgate_hbm, rgate_hbm,
    total_ref, last_ref, lhs_ref,
    idx_ref, lterm_ref, rterm_ref, lgate_ref, rgate_ref,
    lraw, rraw, lx, rx, lt, rt, lsend, early, up, down, peer_blocks, own_blocks, lhs_now,
    in_sem, swap_send, swap_recv,
    ag_send, ag_recv, aa_send, aa_recv, pr_send, pr_recv,
):
    me = lax.axis_index("path")
    core = lax.axis_index("amp")
    nxt, prv = lax.rem(me + 1, chips), lax.rem(me + chips - 1, chips)
    peer = {"amp": 1 - core}
    toward = ({"path": nxt}, {"path": prv})
    half = chips // 2
    pieces, wide = early.shape[1], early.shape[3]
    held = early.shape[0]

    barrier = pltpu.get_barrier_semaphore()
    for who in (peer, *toward):
        pl.semaphore_signal(barrier, inc=1, device_id=who, device_id_type=MESH)
    mine = lx.shape[0]
    loads = [
        pltpu.make_async_copy(src, dst, in_sem.at[n])
        for n, (src, dst) in enumerate((
            (right_hbm, rraw.at[:, core]),
            (rgate_hbm, rgate_ref), (idx_hbm, idx_ref), (rterm_hbm, rterm_ref),
            (lterm_hbm, lterm_ref), (lgate_hbm, lgate_ref),
            (left_hbm.at[pl.ds(core * mine, mine)], lraw.at[:, core])))
    ]
    for load in loads:
        load.start()
    pl.semaphore_wait(barrier, 3)

    rrows, lrows = rx.shape[2] // 2, lx.shape[2] // 2
    give_right = pltpu.make_async_remote_copy(
        src_ref=right_hbm, dst_ref=rraw.at[:, core],
        send_sem=swap_send.at[0], recv_sem=swap_recv.at[0], device_id=peer, device_id_type=MESH)
    give_left = pltpu.make_async_remote_copy(
        src_ref=left_hbm.at[pl.ds((1 - core) * mine, mine)], dst_ref=lraw.at[:, core],
        send_sem=swap_send.at[1], recv_sem=swap_recv.at[1], device_id=peer, device_id_type=MESH)
    give_right.start()
    give_left.start()

    def to_rows(raw, full, part, count):
        @pl.loop(0, raw.shape[0], unroll=4)
        def _(p):
            at = pl.ds(pl.multiple_of(part * count, count), count)
            full[p, :, at] = raw[p, part].reshape(2, count, 128)

    loads[0].wait()
    to_rows(rraw, rx, core, rrows)
    for load in loads[1:4]:
        load.wait()
    row, col = grid2(128, 128)
    pair_swap = one_hot(row == (col ^ 1))
    even = (lax.broadcasted_iota(jnp.int32, (1, 128), 1) & 1) == 0
    prow, pcol = grid2(256, 256)
    regroup = one_hot(pcol == (prow % 8) * 32 + prow // 8)

    s_low = stack_matrix(rgate_ref[0, 0], rgate_ref[0, 1])
    s_low = jnp.concatenate(
        [s_low, s_low[64:128], s_low[0:64], s_low[192:256], s_low[128:192]], 0)
    here = rrows
    full = 2 * here
    srow, scol = grid2(here, 128)
    krow, kcol = grid2(2 * full, 128)
    parts = []
    for c in range(2):
        gate = rgate_ref[1, c]
        rows_of = []
        for t in range(2):
            pick_rows = one_hot(scol == 2 * (core * here + srow) + t)
            pick_cols = one_hot(kcol == 2 * (krow % full) + (krow // full + t) % 2)
            some = dot(pick_rows, gate).astype(BF16)
            rows_of.append(dot(some, pick_cols, NT).astype(BF16))
        parts.append(jnp.concatenate(rows_of, 0))
    s_high = stack_matrix(parts[0], parts[1])

    give_right.wait_recv()
    to_rows(rraw, rx, 1 - core, rrows)
    low_lanes = lax.broadcasted_iota(jnp.int32, (1, 128), 1) < 64
    step = 4
    for first in range(0, rx.shape[0], step):
        cut = cut_paths(rx[first : first + step], first, idx_ref, rterm_ref, pair_swap, even)
        low = dot(cut, s_low, NT).astype(BF16)
        tall = []
        for p in range(step):
            at = low[p * full : (p + 1) * full]
            tall.append(jnp.concatenate(
                [at[:, 0:128], at[:, 256:384], at[:, 128:256], at[:, 384:512]], 0))
        turned = dot(s_high, jnp.concatenate(tall, 1))
        for p in range(step):
            z = turned[:, p * 128 : (p + 1) * 128]
            q = first + p
            for c in range(2):
                at = 2 * c * here
                pair = jnp.where(low_lanes, z[at : at + here], z[at + here : at + 2 * here])
                rt[c, q // 8, (q % 8) * 32 : (q % 8) * 32 + here] = pair.astype(BF16)
    per_piece = here // pieces
    for g in range(2):
        both = [dot(regroup, rt[c, g]) for c in range(2)]
        for r in range(here):
            tile = jnp.concatenate([b[r * 8 : r * 8 + 8] for b in both], 0).astype(BF16)
            at = (r % per_piece) * 128
            early[0, r // per_piece, g * 16 : g * 16 + 16, at : at + 128] = tile

    def slot_of(d, s):
        return min(2 * s - (1 - d), chips - 1) if s else 0

    def right_slot(n):
        return early.at[n] if n < held else last_ref.at[n - held]

    def gather_copy(d, s, j):
        return pltpu.make_async_remote_copy(
            src_ref=right_slot(slot_of(d, s)).at[j], dst_ref=right_slot(slot_of(d, s + 1)).at[j],
            send_sem=ag_send.at[d, s, j], recv_sem=ag_recv.at[d, s, j],
            device_id=toward[d], device_id_type=MESH)

    gather_steps = (half - 1, half)
    group = chips // 4
    quarter = half // 4
    slice_cols = wide // quarter
    lead = pieces // 2

    def add_slice(g, phase, j):
        n = phase * pieces + j
        piece = n // quarter
        first = lax.rem(n, quarter) * slice_cols
        at = pl.ds(pl.multiple_of(first, slice_cols), slice_cols)
        right = early[g * group : (g + 1) * group, piece, :, at].reshape(-1, slice_cols)
        to = pl.ds(pl.multiple_of(n * slice_cols, slice_cols), slice_cols)
        more = dot(lhs_now[...], right)
        total_ref[:, to] = more if g == 0 else total_ref[:, to] + more

    def gather_piece(d, s, j):
        if 1 <= s <= gather_steps[d]:
            gather_copy(d, s - 1, j).wait_recv()
        if s < gather_steps[d]:
            gather_copy(d, s, j).start()

    def gather_half(s, second, work=None):
        @pl.loop(0, lead)
        def _(j):
            gather_piece(0, s, j + lead if second else j)
            gather_piece(1, s + 1 if second else s, j if second else j + lead)
            if work is not None:
                add_slice(*work, j + lead if second else j)

    @pl.loop(0, pieces)
    def _(j):
        for d in range(2):
            gather_piece(d, 0, j)

    for load in loads[4:]:
        load.wait()

    s_low = stack_matrix(lgate_ref[0, 0], lgate_ref[0, 1])
    s_high = stack_matrix(lgate_ref[1, 0], lgate_ref[1, 1])
    give_left.wait_recv()
    for part in range(2):
        to_rows(lraw, lx, part, lrows)
    step = 2
    groups = 4
    for first in range(0, mine, step):
        cut = cut_paths(
            lx[first : first + step], core * mine + first, idx_ref, lterm_ref, pair_swap, even)
        low = dot(cut, s_low, NT).astype(BF16)
        tall = [
            jnp.concatenate([low[p * 128 : (p + 1) * 128, c * 128 : (c + 1) * 128] for c in range(2)], 0)
            for p in range(step)
        ]
        turned = dot(s_high, jnp.concatenate(tall, 1)).astype(BF16)
        for p in range(step):
            for c in range(2):
                for g in range(groups):
                    at = c * 128 + g * 32
                    lt[c, g, (first + p) * 32 : (first + p) * 32 + 32] = (
                        turned[at : at + 32, p * 128 : (p + 1) * 128])
    per_chip = 128 // chips
    for g in range(groups):
        both = [dot(regroup, lt[c, g]) for c in range(2)]
        for r in range(32):
            m = g * 32 + r
            tile = jnp.concatenate([b[r * 8 : r * 8 + 8] for b in both], 0).astype(BF16)
            slot = lax.rem(m // per_chip - me + chips, chips)
            at = (m % per_chip) * 128
            lsend[slot, :, at : at + 128] = tile

    counts = ([half - s for s in range(half)], [half - 1 - s for s in range(half - 1)])
    bases = [[sum(c[:s]) for s in range(len(c))] for c in counts]
    landing = (up, down)

    def block_copy(d, s):
        n = counts[d][s]
        if s == 0:
            src = lsend.at[pl.ds(1, n)] if d == 0 else lsend.at[pl.ds(half + 1, n)]
        else:
            src = landing[d].at[pl.ds(bases[d][s - 1] + (1 if d == 0 else 0), n)]
        return pltpu.make_async_remote_copy(
            src_ref=src, dst_ref=landing[d].at[pl.ds(bases[d][s], n)],
            send_sem=aa_send.at[d, s], recv_sem=aa_recv.at[d, s],
            device_id=toward[d], device_id_type=MESH)

    handed = []

    def hand_over(src, n):
        there = pltpu.make_async_remote_copy(
            src_ref=src, dst_ref=peer_blocks.at[n],
            send_sem=pr_send.at[n], recv_sem=pr_recv.at[n], device_id=peer, device_id_type=MESH)
        there.start()
        handed.append((n, there))
        own_blocks[n] = src[...]

    def block_step(d, s):
        if 1 <= s <= len(counts[d]):
            block_copy(d, s - 1).wait_recv()
        if s < len(counts[d]):
            block_copy(d, s).start()
        if 1 <= s <= len(counts[d]):
            at = bases[d][s - 1] + (0 if d == 0 else counts[d][s - 1] - 1)
            hand_over(landing[d].at[at], slot_of(d, s) if s < half else chips - 1)

    due = {}
    for d in range(2):
        for s in range(1, len(counts[d]) + 1):
            late = s - (half - 3)
            if d == 0:
                when = (s, 1) if late < 0 else ((half - 3, 0), (half - 2, 0), (half - 1, 0), (half - 1, 1))[late]
            else:
                when = (s, 0) if late < 0 else ((half - 4, 1), (half - 3, 1), (half - 2, 1))[late]
            due.setdefault(when, []).append((d, s))

    def pass_blocks(s, part):
        for which in due.get((s, part), ()):
            block_step(*which)

    krow, kcol = grid2(16 * 2 * group, 16 * 2 * group)
    imag = (krow // 8) % 2 == 1
    signed = jnp.where(krow == kcol, jnp.where(imag, -1.0, 1.0), 0.0).astype(BF16)
    crossed = one_hot(krow == (kcol ^ 8))

    def build_lhs(g, to_ref):
        rows = []
        for n in range(g * group, (g + 1) * group):
            dict(handed)[n].wait_recv()
            own, other = own_blocks[n], peer_blocks[n]
            first = core == 0
            rows.append(jnp.where(first, own, other))
            rows.append(jnp.where(first, other, own))
        block = jnp.concatenate(rows, 0)
        to_ref[0 : block.shape[1]] = dot(block, signed, TN).astype(BF16)
        to_ref[block.shape[1] :] = dot(block, crossed, TN).astype(BF16)

    block_step(0, 0)
    hand_over(lsend.at[0], 0)
    block_step(1, 0)

    @pl.loop(0, lead)
    def _(j):
        gather_piece(1, 1, j)

    pass_blocks(0, 1)
    for s in range(1, half):
        ready, phase = divmod(s - 1, quarter)
        if phase == 0 and ready >= 1:
            build_lhs(ready - 1, lhs_now)
        work = (ready - 1, phase) if ready >= 1 else None
        for part in range(2):
            gather_half(s, part, work)
            pass_blocks(s, part)
    ready, phase = divmod(half - 1, quarter)
    if phase == 0:
        build_lhs(ready - 1, lhs_now)

    @pl.loop(0, pieces)
    def _(j):
        add_slice(ready - 1, phase, j)

    build_lhs(3, lhs_ref)
    gather_half(half, 0)

    give_right.wait_send()
    give_left.wait_send()
    for s in range(half):
        @pl.loop(0, pieces)
        def _(j):
            for d in range(2):
                if s < gather_steps[d]:
                    gather_copy(d, s, j).wait_send()
        for d in range(2):
            if s < len(counts[d]):
                block_copy(d, s).wait_send()
    for _, there in handed:
        there.wait_send()


def finish_kernel(total_ref, last_ref, lhs_ref, out_ref, staged, sems):
    count, _, rows, tile = staged.shape
    per = last_ref.shape[3] // tile

    def put(k):
        to = pl.ds(pl.multiple_of(k * tile, tile), tile)
        return pltpu.make_async_copy(staged.at[k], out_ref.at[:, :, to], sems.at[k])

    @pl.loop(0, count)
    def _(k):
        at = pl.ds(pl.multiple_of(lax.rem(k, per) * tile, tile), tile)
        right = last_ref[:, k // per, :, at].reshape(-1, tile)
        to = pl.ds(pl.multiple_of(k * tile, tile), tile)
        for c in range(2):
            part = slice(c * rows, (c + 1) * rows)
            staged[k, c] = (total_ref[part, to] + dot(lhs_ref[part], right)).astype(BF16)
        put(k).start()

    @pl.loop(0, count)
    def _(k):
        put(k).wait()


def shards(left_slabs, right_slabs, term_index, left_terms, right_terms, left_gates, right_gates):
    chips = lax.axis_size("path")
    paths = left_slabs.shape[0]
    mine = paths // 2
    lrows, rrows = left_slabs.shape[2] // 128, right_slabs.shape[2] // 128
    half = chips // 2
    pieces = PIECES
    cols = rrows * 128
    block = 2 * lrows * 128 // chips
    vmem = pl.BlockSpec(memory_space=pltpu.VMEM)
    hbm = pl.BlockSpec(memory_space=pltpu.HBM)
    dma = pltpu.SemaphoreType.DMA
    held = chips // 4 * 3
    wide = cols // pieces
    depth = chips // 4 * 2 * paths
    blocks = (2 * mine, block)
    total, last, lhs = pl.pallas_call(
        functools.partial(exchange_kernel, chips),
        out_shape=(
            jax.ShapeDtypeStruct((2 * block, cols), F32),
            jax.ShapeDtypeStruct((chips - held, pieces, 2 * paths, wide), BF16),
            jax.ShapeDtypeStruct((2 * block, depth), BF16),
        ),
        in_specs=[hbm] * 7,
        out_specs=(vmem, vmem, vmem),
        scratch_shapes=[
            pltpu.SMEM((paths,), jnp.int32),
            pltpu.SMEM((2, 2, 2, 4), F32),
            pltpu.SMEM((2, 2, 2, 4), F32),
            pltpu.VMEM(left_gates.shape, BF16),
            pltpu.VMEM(right_gates.shape, BF16),
            pltpu.VMEM((mine, 2, 2, lrows * 128), BF16),
            pltpu.VMEM((paths, 2, 2, rrows * 128), BF16),
            pltpu.VMEM((mine, 2, 2 * lrows, 128), BF16),
            pltpu.VMEM((paths, 2, 2 * rrows, 128), BF16),
            pltpu.VMEM((2, 4, 256, 128), BF16),
            pltpu.VMEM((2, 2, 256, 128), BF16),
            pltpu.VMEM((chips, *blocks), BF16),
            pltpu.VMEM((held, pieces, 2 * paths, wide), BF16),
            pltpu.VMEM((half * (half + 1) // 2, *blocks), BF16),
            pltpu.VMEM((half * (half - 1) // 2, *blocks), BF16),
            pltpu.VMEM((chips, *blocks), BF16),
            pltpu.VMEM((chips, *blocks), BF16),
            pltpu.VMEM((2 * block, depth), BF16),
            dma((7,)), dma((2,)), dma((2,)),
            dma((2, half, pieces)), dma((2, half, pieces)),
            dma((2, half)), dma((2, half)),
            dma((chips,)), dma((chips,)),
        ],
        compiler_params=pltpu.CompilerParams(
            collective_id=0, has_side_effects=True, vmem_limit_bytes=VMEM_LIMIT),
        name="exchange",
    )(
        *(pltpu.with_memory_space_constraint(x, pltpu.HBM) for x in (
            term_index, jnp.transpose(left_terms, (1, 2, 3, 0)), jnp.transpose(right_terms, (1, 2, 3, 0)),
            left_slabs, right_slabs, left_gates, right_gates)),
    )
    tile = min(512, wide)
    return pl.pallas_call(
        finish_kernel,
        out_shape=jax.ShapeDtypeStruct((2, block, cols), BF16),
        in_specs=[vmem, vmem, vmem],
        out_specs=hbm,
        scratch_shapes=[
            pltpu.VMEM((cols // tile, 2, block, tile), BF16),
            pltpu.SemaphoreType.DMA((cols // tile,)),
        ],
        compiler_params=pltpu.CompilerParams(vmem_limit_bytes=16 * 1024 * 1024),
        name="finish",
    )(total, last, lhs)


def solution(mesh):
    return jax.shard_map(
        shards,
        mesh=mesh,
        in_specs=(
            P(("grp", "path"), None, "amp"),
            P(("grp", "path"), None, "amp"),
            P(("grp", "path")),
            P(),
            P(),
            P(),
            P(),
        ),
        out_specs=P(None, ("grp", "path"), "amp"),
        check_vma=False,
    )
```
